32 devices in a mesh: blk: 8 (over z, x), grp: 4 (over y, core).
Axes of the slice: x: 2, y: 2, z: 4, core: 2. Of those that a mesh axis runs over, the one named last changes fastest.
Arguments:
- amplitudes: bfloat16 [8, 512, 1024], P('blk', None, 'grp'), may hold values from -6 to 6
- integrals: bfloat16 [64, 1024, 1024], P('blk', 'grp'), may hold values from -0.1875 to 0.1875
- cd_index: int32 [64], replicated, may hold values from 0 to 7, as said below
- live_blocks: int32 [8], replicated, may hold values from 4 to 8, as said below
- occ_energy: float32 [512], P('grp'), may hold values from -3 to -0.5
- vir_energy: float32 [8, 1024], P('blk'), may hold values from 0.5 to 4
Outputs:
- amplitude_step: float32 [8, 512, 1024], P('blk', 'grp')
The draws below stay inside these ranges and needn't reach their ends.
Inputs may be any that keep to these rules, and one draw needn't show every extreme that they name: (cd_index[k] - k // 8) mod 8 is at most 2 or at least 6; among the first 4 slots of each pair block every nonzero offset from -2 to 2 occurs once. `live_blocks`: 8 is reached by some pair block in every draw.
All inputs are finite; a program needn't handle non-finite values.
Results may differ from the reference program's by a relative error of at most 0.0003.
Values may be sent and summed in bfloat16 or wider, within the bound.
A program may use at most 64 MiB of HBM per device.

```python
import jax
import jax.numpy as jnp
from jax import lax

PW = 1024
OCC = 512
INT_DEV = 8
REACH = 2
NPB = 8
NINT = 64


def draw_cd_index(key, part):
    key_list = jax.random.split(jax.random.fold_in(key, 11), 2)
    shifts = jax.random.randint(key_list[0], (NPB, INT_DEV), -REACH, REACH + 1).astype(jnp.int32)
    rotation = jax.random.randint(key_list[1], (NPB, 1), 0, 2 * REACH).astype(jnp.int32)
    slot_ids = jnp.arange(INT_DEV, dtype=jnp.int32)[None, :]
    cycled = jnp.mod(slot_ids + rotation, 2 * REACH)
    covered = cycled - REACH + (cycled >= REACH).astype(jnp.int32)
    shifts = jnp.where(slot_ids < 2 * REACH, covered, shifts)
    owners = jnp.arange(NPB, dtype=jnp.int32)[:, None]
    return jnp.mod(owners + shifts, NPB).reshape(NINT).astype(jnp.int32)


def draw_live_blocks(key, part):
    key_list = jax.random.split(jax.random.fold_in(key, 23), 3)
    base_live = jax.random.randint(key_list[0], (NPB,), 2 * REACH, 2 * REACH + 2)
    base_live = jnp.minimum(base_live, INT_DEV)
    heavy_rows = jax.random.randint(key_list[1], (NPB,), 0, 8) == 0
    live_counts = jnp.where(heavy_rows, INT_DEV, base_live)
    full_row = jax.random.randint(key_list[2], (), 0, NPB)
    return live_counts.at[full_row].set(INT_DEV).astype(jnp.int32)


def block_levels(stream_key, extent, pieces, least, top_value):
    def one(axis_at, blocks):
        heights = jax.random.uniform(jax.random.fold_in(jax.random.fold_in(stream_key, 6), axis_at), (blocks,), jnp.float32, least / len(pieces), top_value / len(pieces))
        return jnp.repeat(jnp.exp(heights), extent[axis_at] // blocks).reshape((-1,) + (1,) * (len(extent) - axis_at - 1))

    factor_of = one(*pieces[0])
    for cut in pieces[1:]:
        factor_of = factor_of * one(*cut)
    return factor_of


def bell_draw(own_key, extent, width, bound, cuts=(), held_as=jnp.bfloat16):
    array = jax.random.normal(own_key, extent, jnp.float32) * width
    if len(cuts) > 0:
        array = block_levels(own_key, extent, cuts, -0.22, 0.18) * array
    return jnp.clip(array, min=-bound, max=bound).astype(held_as)


def setup_inputs(seed: int = 0) -> dict:
    keys = jax.random.split(jax.random.key(seed), 7)
    return {
        "amplitudes": bell_draw(keys[0], (NPB, OCC, PW), 1.0, 6.0, ((0, 8), (2, 4))),
        "integrals": bell_draw(keys[1], (NINT, PW, PW), PW ** -0.5, 0.1875, ((0, 8), (1, 4))),
        "cd_index": draw_cd_index(jax.random.fold_in(keys[6], 71), 0),
        "live_blocks": draw_live_blocks(jax.random.fold_in(keys[6], 71), 0),
        "occ_energy": jnp.clip(-3.0 + 2.5 * jax.random.uniform(keys[4], (OCC,), jnp.float32) ** block_levels(keys[4], (OCC,), ((0, 4),), -0.2, 0.2), -3.0, -0.5),
        "vir_energy": jnp.clip(0.5 + 3.5 * jax.random.uniform(keys[5], (NPB, PW), jnp.float32) ** block_levels(keys[5], (NPB, PW), ((0, 8),), -0.2, 0.2), 0.5, 4.0),
    }


def reference(amplitudes, integrals, cd_index, live_blocks, occ_energy, vir_energy):
    def one_block(block_index):
        def add_task(running, slot_index):
            task_index = block_index * INT_DEV + slot_index

            def product(running):
                amp_block = amplitudes[cd_index[task_index]]
                return running + jnp.dot(amp_block, integrals[task_index], preferred_element_type=jnp.float32)

            def unchanged(running):
                return running

            return lax.cond(slot_index < live_blocks[block_index], product, unchanged, running), None

        start_sum = jnp.zeros((OCC, PW), jnp.float32)
        ladder, _ = lax.scan(add_task, start_sum, jnp.arange(INT_DEV, dtype=jnp.int32))
        denominator = vir_energy[block_index][None, :] - occ_energy[:, None]
        return ladder / denominator

    return lax.map(one_block, jnp.arange(NPB, dtype=jnp.int32))
```

```python
import functools

import jax
import jax.numpy as jnp
from jax import lax
from jax.experimental import pallas as pl
from jax.experimental.pallas import tpu as pltpu
from jax.sharding import PartitionSpec as P

REACH = 2
PIECES = 2
TILE = 256
MESH = pl.DeviceIdType.MESH


def ladder_kernel(blocks, groups, cd_ref, live_ref, amp_ref, int_ref, out_ref, *scratch):
    slots, depth, cols = int_ref.shape
    rows = amp_ref.shape[1]
    halves = groups // 2
    owned = rows // groups
    piece = owned // PIECES
    steps = halves * PIECES
    far_steps = steps - PIECES
    window = 2 * REACH + 1
    near = scratch[:steps]
    (weights, own, pair_out, pair_in, far_out, far_in,
     amp_sem, int_sem, amp_send, amp_recv, pair_send, pair_recv, far_send, far_recv) = scratch[steps:]

    here = lax.axis_index("blk")
    me = lax.axis_index("grp")
    half, core = me // 2, me % 2
    mate = half * 2 + 1 - core
    offsets = [o for d in range(1, REACH + 1) for o in (d, -d)]

    amp_loads = []
    for step in range(steps):
        there = (half + step // PIECES + 1) % halves
        for part, side in enumerate((1 - core, core)):
            start = pl.multiple_of((there * 2 + side) * owned + (step % PIECES) * piece, piece)
            amp_loads.append(pltpu.make_async_copy(
                amp_ref.at[0, pl.ds(start, piece)],
                near[step].at[REACH, pl.ds(part * piece, piece)],
                amp_sem.at[step, part]))
    int_loads = [pltpu.make_async_copy(int_ref.at[k], weights.at[pl.ds(k * depth, depth)], int_sem.at[k])
                 for k in range(slots)]
    for load in amp_loads:
        load.start()
    for load in int_loads:
        load.start()

    barrier = pltpu.get_barrier_semaphore()
    for offset in offsets:
        pl.semaphore_signal(barrier, inc=1, device_id={"blk": (here - offset + blocks) % blocks}, device_id_type=MESH)
    pl.semaphore_signal(barrier, inc=1, device_id={"grp": mate}, device_id_type=MESH)
    for hop in range(1, halves):
        pl.semaphore_signal(barrier, inc=1, device_id={"grp": (half + hop) % halves * 2 + core}, device_id_type=MESH)
    for step in range(steps):
        near[step][window] = jnp.zeros(near[step].shape[1:], near[step].dtype)
    for load in amp_loads:
        load.wait()
    pl.semaphore_wait(barrier, len(offsets) + halves)

    amp_copies = {}
    for step in range(steps):
        for i, offset in enumerate(offsets):
            copy = pltpu.make_async_remote_copy(
                near[step].at[REACH], near[step].at[REACH + offset],
                amp_send.at[i, step], amp_recv.at[i, step],
                device_id={"blk": (here - offset + blocks) % blocks}, device_id_type=MESH)
            copy.start()
            amp_copies[i, step] = copy

    picks = []
    for k in range(slots):
        offset = (cd_ref[here * slots + k] - here + REACH + blocks) % blocks
        picks.append(jnp.where(k < live_ref[here], offset, window))

    pair_copies, far_copies = [], []

    def settle(step):
        pair_copies[step].wait_recv()
        if step < far_steps:
            far_out[step] = own[step] + pair_in[step]
            there = (half + step // PIECES + 1) % halves * 2 + core
            copy = pltpu.make_async_remote_copy(
                far_out.at[step], far_in.at[step], far_send.at[step], far_recv.at[step],
                device_id={"grp": there}, device_id_type=MESH)
            copy.start()
            far_copies.append(copy)

    for load in int_loads:
        load.wait()
    for step in range(steps):
        for i in range(len(offsets)):
            amp_copies[i, step].wait_recv()
        lhs = jnp.concatenate([near[step][pick] for pick in picks], axis=1)

        @pl.loop(0, cols // TILE)
        def _(tile):
            lanes = pl.ds(pl.multiple_of(tile * TILE, TILE), TILE)
            product = jnp.dot(lhs, weights[:, lanes], preferred_element_type=jnp.float32)
            pair_out[step, :, lanes] = product[:piece]
            own[step, :, lanes] = product[piece:]

        copy = pltpu.make_async_remote_copy(
            pair_out.at[step], pair_in.at[step], pair_send.at[step], pair_recv.at[step],
            device_id={"grp": mate}, device_id_type=MESH)
        copy.start()
        pair_copies.append(copy)
        if step >= 1:
            settle(step - 1)
    settle(steps - 1)
    for part in range(PIECES):
        total = own[far_steps + part] + pair_in[far_steps + part]
        for hop in range(halves - 1):
            far_copies[hop * PIECES + part].wait_recv()
            total = total + far_in[hop * PIECES + part]
        out_ref[pl.ds(part * piece, piece)] = total
    for copy in list(amp_copies.values()) + pair_copies + far_copies:
        copy.wait_send()


def body(blocks, groups, amplitudes, integrals, cd_index, live_blocks, occ_energy, vir_energy):
    slots, depth, cols = integrals.shape
    rows = amplitudes.shape[1]
    owned = rows // groups
    piece = owned // PIECES
    steps = groups // 2 * PIECES
    far_steps = steps - PIECES
    window = 2 * REACH + 1
    ladder = pl.pallas_call(
        functools.partial(ladder_kernel, blocks, groups),
        out_shape=jax.ShapeDtypeStruct((owned, cols), jnp.float32),
        in_specs=[pl.BlockSpec(memory_space=pltpu.SMEM)] * 2 + [pl.BlockSpec(memory_space=pl.ANY)] * 2,
        out_specs=pl.BlockSpec(memory_space=pltpu.VMEM),
        scratch_shapes=[pltpu.VMEM((window + 1, 2 * piece, depth), amplitudes.dtype)] * steps + [
            pltpu.VMEM((slots * depth, cols), integrals.dtype),
            pltpu.VMEM((steps, piece, cols), jnp.float32),
            pltpu.VMEM((steps, piece, cols), jnp.float32),
            pltpu.VMEM((steps, piece, cols), jnp.float32),
            pltpu.VMEM((far_steps, piece, cols), jnp.float32),
            pltpu.VMEM((far_steps, piece, cols), jnp.float32),
            pltpu.SemaphoreType.DMA((steps, 2)),
            pltpu.SemaphoreType.DMA((slots,)),
            pltpu.SemaphoreType.DMA((2 * REACH, steps)),
            pltpu.SemaphoreType.DMA((2 * REACH, steps)),
            pltpu.SemaphoreType.DMA((steps,)),
            pltpu.SemaphoreType.DMA((steps,)),
            pltpu.SemaphoreType.DMA((far_steps,)),
            pltpu.SemaphoreType.DMA((far_steps,)),
        ],
        compiler_params=pltpu.CompilerParams(
            collective_id=0, has_side_effects=True, vmem_limit_bytes=24 * 1024 * 1024),
    )(cd_index, live_blocks, amplitudes, integrals)
    denominator = vir_energy[0][None, :] - occ_energy[:, None]
    return (ladder / denominator)[None]


def solution(mesh):
    return jax.shard_map(
        functools.partial(body, mesh.shape["blk"], mesh.shape["grp"]),
        mesh=mesh,
        in_specs=(P("blk", None, "grp"), P("blk", "grp", None), P(), P(), P("grp"), P("blk", None)),
        out_specs=P("blk", "grp", None),
        check_vma=False,
    )
```

```python
import functools

import jax
import jax.numpy as jnp
from jax import lax
from jax.experimental import pallas as pl
from jax.experimental.pallas import tpu as pltpu
from jax.sharding import PartitionSpec as P

REACH = 2
PIECES = 4
AHEAD = 2
TILE = 256
MESH = pl.DeviceIdType.MESH


def ladder_kernel(blocks, groups, cd_ref, live_ref, amp_ref, int_ref, out_ref, *scratch):
    slots, depth, cols = int_ref.shape
    rows = amp_ref.shape[1]
    halves = groups // 2
    owned = rows // groups
    piece = owned // PIECES
    steps = halves * PIECES
    far_steps = steps - PIECES
    window = 2 * REACH + 1
    near = scratch[:steps]
    (cd_smem, live_smem, table_sem, weights, own, pair_out, pair_in, far_out, far_in,
     amp_sem, int_sem, amp_send, amp_recv, pair_send, pair_recv, far_send, far_recv) = scratch[steps:]

    here = lax.axis_index("blk")
    me = lax.axis_index("grp")
    half, core = me // 2, me % 2
    mate = half * 2 + 1 - core
    side = 1 - 2 * (here % 2)
    twin = here + side

    amp_loads = []
    for step in range(steps):
        there = (half + step // PIECES + 1) % halves
        for part, lane in enumerate((1 - core, core)):
            start = pl.multiple_of((there * 2 + lane) * owned + (step % PIECES) * piece, piece)
            amp_loads.append(pltpu.make_async_copy(
                amp_ref.at[0, pl.ds(start, piece)],
                near[step].at[REACH, pl.ds(part * piece, piece)],
                amp_sem.at[step, part]))
    int_loads = [pltpu.make_async_copy(int_ref.at[k], weights.at[pl.ds(k * depth, depth)], int_sem.at[k])
                 for k in range(slots)]
    table_loads = [pltpu.make_async_copy(cd_ref, cd_smem, table_sem.at[0]),
                   pltpu.make_async_copy(live_ref, live_smem, table_sem.at[1])]
    for load in amp_loads + int_loads + table_loads:
        load.start()

    up, down = (here + REACH) % blocks, (here - REACH + blocks) % blocks
    barrier = pltpu.get_barrier_semaphore()
    for target in (up, down, twin):
        pl.semaphore_signal(barrier, inc=1, device_id={"blk": target}, device_id_type=MESH)
    pl.semaphore_signal(barrier, inc=1, device_id={"grp": mate}, device_id_type=MESH)
    for hop in range(1, halves):
        pl.semaphore_signal(barrier, inc=1, device_id={"grp": (half + hop) % halves * 2 + core}, device_id_type=MESH)
    for step in range(steps):
        near[step][window] = jnp.zeros(near[step].shape[1:], near[step].dtype)
    for load in amp_loads:
        load.wait()
    pl.semaphore_wait(barrier, 3 + halves)

    def push(step, source, slot, lane, target):
        return pltpu.make_async_remote_copy(
            near[step].at[source], near[step].at[slot], amp_send.at[lane, step], amp_recv.at[slot, step],
            device_id={"blk": target}, device_id_type=MESH)

    def arrival(step, slot):
        push(step, REACH, slot, 0, up).wait_recv()

    sent = []

    def launch(copy):
        copy.start()
        sent.append(copy)

    def push_twin(step):
        if step < steps:
            launch(push(step, REACH, REACH - side, 2, twin))

    def forward(step):
        if step < steps:
            arrival(step, REACH + 2 * side)
            launch(push(step, REACH + 2 * side, REACH + side, 3, twin))
            push_twin(step + AHEAD)

    for step in range(steps):
        launch(push(step, REACH, 0, 0, up))
        launch(push(step, REACH, 2 * REACH, 1, down))
        if step < AHEAD:
            push_twin(step)

    for load in table_loads:
        load.wait()
    picks = []
    for k in range(slots):
        offset = (cd_smem[here * slots + k] - here + REACH + blocks) % blocks
        picks.append(jnp.where(k < live_smem[here], offset, window))

    pair_copies, far_copies = [], []

    def settle(step):
        pair_copies[step].wait_recv()
        if step < far_steps:
            far_out[step] = own[step] + pair_in[step]
            there = (half + step // PIECES + 1) % halves * 2 + core
            copy = pltpu.make_async_remote_copy(
                far_out.at[step], far_in.at[step], far_send.at[step], far_recv.at[step],
                device_id={"grp": there}, device_id_type=MESH)
            copy.start()
            far_copies.append(copy)

    for load in int_loads:
        load.wait()
    forward(0)
    for step in range(steps):
        forward(step + 1)
        for slot in (REACH - 2 * side, REACH - side, REACH + side):
            arrival(step, slot)
        lhs = jnp.concatenate([near[step][pick] for pick in picks], axis=1)

        @pl.loop(0, cols // TILE)
        def _(tile):
            lanes = pl.ds(pl.multiple_of(tile * TILE, TILE), TILE)
            product = jnp.dot(lhs, weights[:, lanes], preferred_element_type=jnp.float32)
            pair_out[step, :, lanes] = product[:piece]
            own[step, :, lanes] = product[piece:]

        copy = pltpu.make_async_remote_copy(
            pair_out.at[step], pair_in.at[step], pair_send.at[step], pair_recv.at[step],
            device_id={"grp": mate}, device_id_type=MESH)
        copy.start()
        pair_copies.append(copy)
        if step >= 1:
            settle(step - 1)
    settle(steps - 1)
    for part in range(PIECES):
        total = own[far_steps + part] + pair_in[far_steps + part]
        for hop in range(halves - 1):
            far_copies[hop * PIECES + part].wait_recv()
            total = total + far_in[hop * PIECES + part]
        out_ref[pl.ds(part * piece, piece)] = total
    for copy in sent + pair_copies + far_copies:
        copy.wait_send()


def body(blocks, groups, amplitudes, integrals, cd_index, live_blocks, occ_energy, vir_energy):
    slots, depth, cols = integrals.shape
    rows = amplitudes.shape[1]
    owned = rows // groups
    piece = owned // PIECES
    steps = groups // 2 * PIECES
    far_steps = steps - PIECES
    window = 2 * REACH + 1
    ladder = pl.pallas_call(
        functools.partial(ladder_kernel, blocks, groups),
        out_shape=jax.ShapeDtypeStruct((owned, cols), jnp.float32),
        in_specs=[pl.BlockSpec(memory_space=pltpu.HBM)] * 4,
        out_specs=pl.BlockSpec(memory_space=pltpu.VMEM),
        scratch_shapes=[pltpu.VMEM((window + 1, 2 * piece, depth), amplitudes.dtype)] * steps + [
            pltpu.SMEM(cd_index.shape, cd_index.dtype),
            pltpu.SMEM(live_blocks.shape, live_blocks.dtype),
            pltpu.SemaphoreType.DMA((2,)),
            pltpu.VMEM((slots * depth, cols), integrals.dtype),
            pltpu.VMEM((steps, piece, cols), jnp.float32),
            pltpu.VMEM((steps, piece, cols), jnp.float32),
            pltpu.VMEM((steps, piece, cols), jnp.float32),
            pltpu.VMEM((far_steps, piece, cols), jnp.float32),
            pltpu.VMEM((far_steps, piece, cols), jnp.float32),
            pltpu.SemaphoreType.DMA((steps, 2)),
            pltpu.SemaphoreType.DMA((slots,)),
            pltpu.SemaphoreType.DMA((4, steps)),
            pltpu.SemaphoreType.DMA((window, steps)),
            pltpu.SemaphoreType.DMA((steps,)),
            pltpu.SemaphoreType.DMA((steps,)),
            pltpu.SemaphoreType.DMA((far_steps,)),
            pltpu.SemaphoreType.DMA((far_steps,)),
        ],
        compiler_params=pltpu.CompilerParams(
            collective_id=0, has_side_effects=True, vmem_limit_bytes=24 * 1024 * 1024),
    )(*[pltpu.with_memory_space_constraint(x, pltpu.HBM) for x in (cd_index, live_blocks, amplitudes, integrals)])
    denominator = vir_energy[0][None, :] - occ_energy[:, None]
    return (ladder / denominator)[None]


def solution(mesh):
    return jax.shard_map(
        functools.partial(body, mesh.shape["blk"], mesh.shape["grp"]),
        mesh=mesh,
        in_specs=(P("blk", None, "grp"), P("blk", "grp", None), P(), P(), P("grp"), P("blk", None)),
        out_specs=P("blk", "grp", None),
        check_vma=False,
    )
```

```python
import functools

import jax
import jax.numpy as jnp
from jax import lax
from jax.experimental import pallas as pl
from jax.experimental.pallas import tpu as pltpu
from jax.sharding import PartitionSpec as P

REACH = 2
PIECES = 4
AHEAD = 2
TILE = 512
MESH = pl.DeviceIdType.MESH


def ladder_kernel(blocks, groups, cd_ref, live_ref, amp_ref, int_ref, out_ref, *scratch):
    slots, depth, cols = int_ref.shape
    rows = amp_ref.shape[1]
    halves = groups // 2
    owned = rows // groups
    piece = owned // PIECES
    steps = halves * PIECES
    far_steps = steps - PIECES
    window = 2 * REACH + 1
    near = scratch[:steps]
    (cd_smem, live_smem, table_sem, weights, own, pair_out, pair_in, far_out, far_in,
     amp_sem, int_sem, amp_send, amp_recv, pair_send, pair_recv, far_send, far_recv) = scratch[steps:]

    here = lax.axis_index("blk")
    me = lax.axis_index("grp")
    half, core = me // 2, me % 2
    mate = half * 2 + 1 - core
    side = 1 - 2 * (here % 2)
    twin = here + side

    amp_loads = []
    for step in range(steps):
        there = (half + step // PIECES + 1) % halves
        for part, lane in enumerate((1 - core, core)):
            start = pl.multiple_of((there * 2 + lane) * owned + (step % PIECES) * piece, piece)
            amp_loads.append(pltpu.make_async_copy(
                amp_ref.at[0, pl.ds(start, piece)],
                near[step].at[REACH, pl.ds(part * piece, piece)],
                amp_sem.at[step, part]))
    int_loads = [pltpu.make_async_copy(int_ref.at[k], weights.at[pl.ds(k * depth, depth)], int_sem.at[k])
                 for k in range(slots)]
    table_loads = [pltpu.make_async_copy(cd_ref, cd_smem, table_sem.at[0]),
                   pltpu.make_async_copy(live_ref, live_smem, table_sem.at[1])]
    for load in amp_loads + int_loads + table_loads:
        load.start()

    up, down = (here + REACH) % blocks, (here - REACH + blocks) % blocks
    barrier = pltpu.get_barrier_semaphore()
    for target in (up, down, twin):
        pl.semaphore_signal(barrier, inc=1, device_id={"blk": target}, device_id_type=MESH)
    pl.semaphore_signal(barrier, inc=1, device_id={"grp": mate}, device_id_type=MESH)
    for hop in range(1, halves):
        pl.semaphore_signal(barrier, inc=1, device_id={"grp": (half + hop) % halves * 2 + core}, device_id_type=MESH)
    for step in range(steps):
        near[step][window] = jnp.zeros(near[step].shape[1:], near[step].dtype)
    for load in amp_loads:
        load.wait()
    pl.semaphore_wait(barrier, 3 + halves)

    def push(step, source, slot, lane, target):
        return pltpu.make_async_remote_copy(
            near[step].at[source], near[step].at[slot], amp_send.at[lane, step], amp_recv.at[slot, step],
            device_id={"blk": target}, device_id_type=MESH)

    def arrival(step, slot):
        push(step, REACH, slot, 0, up).wait_recv()

    sent = []

    def launch(copy):
        copy.start()
        sent.append(copy)

    def push_twin(step):
        if step < steps:
            launch(push(step, REACH, REACH - side, 2, twin))

    def forward(step):
        if step < steps:
            arrival(step, REACH + 2 * side)
            launch(push(step, REACH + 2 * side, REACH + side, 3, twin))
            push_twin(step + AHEAD)

    for step in range(steps):
        launch(push(step, REACH, 0, 0, up))
        launch(push(step, REACH, 2 * REACH, 1, down))
        if step < AHEAD:
            push_twin(step)

    for load in table_loads:
        load.wait()
    picks = []
    for k in range(slots):
        offset = (cd_smem[here * slots + k] - here + REACH + blocks) % blocks
        picks.append(jnp.where(k < live_smem[here], offset, window))

    pair_copies, far_copies = [], []

    def settle(step):
        pair_copies[step].wait_recv()
        if step < far_steps:
            far_out[step] = own[step] + pair_in[step]
            there = (half + step // PIECES + 1) % halves * 2 + core
            copy = pltpu.make_async_remote_copy(
                far_out.at[step], far_in.at[step], far_send.at[step], far_recv.at[step],
                device_id={"grp": there}, device_id_type=MESH)
            copy.start()
            far_copies.append(copy)

    for load in int_loads:
        load.wait()
    forward(0)
    for step in range(steps):
        forward(step + 1)
        for slot in (REACH - 2 * side, REACH - side, REACH + side):
            arrival(step, slot)
        lhs = jnp.concatenate([near[step][pick] for pick in picks], axis=1)

        @pl.loop(0, cols // TILE)
        def _(tile):
            lanes = pl.ds(pl.multiple_of(tile * TILE, TILE), TILE)
            product = jnp.dot(lhs, weights[:, lanes], preferred_element_type=jnp.float32)
            pair_out[step, :, lanes] = product[:piece]
            own[step, :, lanes] = product[piece:]

        copy = pltpu.make_async_remote_copy(
            pair_out.at[step], pair_in.at[step], pair_send.at[step], pair_recv.at[step],
            device_id={"grp": mate}, device_id_type=MESH)
        copy.start()
        pair_copies.append(copy)
        if step >= 1:
            settle(step - 1)
    settle(steps - 1)
    for part in range(PIECES):
        total = own[far_steps + part] + pair_in[far_steps + part]
        for hop in range(halves - 1):
            far_copies[hop * PIECES + part].wait_recv()
            total = total + far_in[hop * PIECES + part]
        out_ref[pl.ds(part * piece, piece)] = total
    for copy in sent + pair_copies + far_copies:
        copy.wait_send()


def body(blocks, groups, amplitudes, integrals, cd_index, live_blocks, occ_energy, vir_energy):
    slots, depth, cols = integrals.shape
    rows = amplitudes.shape[1]
    owned = rows // groups
    piece = owned // PIECES
    steps = groups // 2 * PIECES
    far_steps = steps - PIECES
    window = 2 * REACH + 1
    ladder = pl.pallas_call(
        functools.partial(ladder_kernel, blocks, groups),
        out_shape=jax.ShapeDtypeStruct((owned, cols), jnp.float32),
        in_specs=[pl.BlockSpec(memory_space=pltpu.HBM)] * 4,
        out_specs=pl.BlockSpec(memory_space=pltpu.VMEM),
        scratch_shapes=[pltpu.VMEM((window + 1, 2 * piece, depth), amplitudes.dtype)] * steps + [
            pltpu.SMEM(cd_index.shape, cd_index.dtype),
            pltpu.SMEM(live_blocks.shape, live_blocks.dtype),
            pltpu.SemaphoreType.DMA((2,)),
            pltpu.VMEM((slots * depth, cols), integrals.dtype),
            pltpu.VMEM((steps, piece, cols), jnp.float32),
            pltpu.VMEM((steps, piece, cols), jnp.float32),
            pltpu.VMEM((steps, piece, cols), jnp.float32),
            pltpu.VMEM((far_steps, piece, cols), jnp.float32),
            pltpu.VMEM((far_steps, piece, cols), jnp.float32),
            pltpu.SemaphoreType.DMA((steps, 2)),
            pltpu.SemaphoreType.DMA((slots,)),
            pltpu.SemaphoreType.DMA((4, steps)),
            pltpu.SemaphoreType.DMA((window, steps)),
            pltpu.SemaphoreType.DMA((steps,)),
            pltpu.SemaphoreType.DMA((steps,)),
            pltpu.SemaphoreType.DMA((far_steps,)),
            pltpu.SemaphoreType.DMA((far_steps,)),
        ],
        compiler_params=pltpu.CompilerParams(
            collective_id=0, has_side_effects=True, vmem_limit_bytes=24 * 1024 * 1024),
    )(*[pltpu.with_memory_space_constraint(x, pltpu.HBM) for x in (cd_index, live_blocks, amplitudes, integrals)])
    denominator = vir_energy[0][None, :] - occ_energy[:, None]
    return (ladder / denominator)[None]


def solution(mesh):
    return jax.shard_map(
        functools.partial(body, mesh.shape["blk"], mesh.shape["grp"]),
        mesh=mesh,
        in_specs=(P("blk", None, "grp"), P("blk", "grp", None), P(), P(), P("grp"), P("blk", None)),
        out_specs=P("blk", "grp", None),
        check_vma=False,
    )
```
